32 devices in a mesh: data: 1 (over z), group: 32 (over y, x, core).
Axes of the slice: x: 4, y: 4, z: 1, core: 2. Of those that a mesh axis runs over, the one named last changes fastest.
The devices are a block of a 4x4x8 slice.
Arguments:
- latents: bfloat16 [4096, 1152], P(('data', 'group'))
- hint_embed: bfloat16 [4096, 1152], P(('data', 'group'))
- in_qkv: bfloat16 [2, 3, 1152, 3456], replicated
- in_proj: bfloat16 [2, 3, 16, 72, 1152], replicated
- in_up: bfloat16 [2, 3, 1152, 4608], replicated
- in_down: bfloat16 [2, 3, 4608, 1152], replicated
- in_norm: bfloat16 [2, 3, 4, 1152], replicated
- out_qkv: bfloat16 [2, 1152, 3456], replicated
- out_proj: bfloat16 [2, 16, 72, 1152], replicated
- out_up: bfloat16 [2, 1152, 4608], replicated
- out_down: bfloat16 [2, 4608, 1152], replicated
- out_norm: bfloat16 [2, 4, 1152], replicated
- zero_proj: bfloat16 [3, 1152, 1152], replicated
- hint_proj: bfloat16 [1152, 1152], replicated
- skip_proj: bfloat16 [2, 2304, 1152], replicated
- final_norm: bfloat16 [2, 1152], replicated
- w_out: bfloat16 [1152, 1152], replicated
Outputs:
- output: bfloat16 [4096, 1152], P(('data', 'group'))
All inputs are finite; a program needn't handle non-finite values.
Results may differ from the reference program's by a relative error of at most 0.02.
Values are sent between devices in bfloat16 or wider.
A program may use at most 768 MiB of HBM per device.

```python
import math
import jax
import jax.numpy as jnp
from jax import lax

TOKENS = 4096
WIDTH = 1152
HEADS = 16
LAYERS = 2

HEAD_DIM = WIDTH // HEADS
IN_BLOCKS = LAYERS + 1
Q_GAIN = math.sqrt(max(1.0, math.log(TOKENS / 16.0)))
EPS = 1e-6


def draw_normal(rng_key, dim_sizes, std_scale):
    return (jax.random.normal(rng_key, dim_sizes, jnp.float32) * std_scale).astype(jnp.bfloat16)


def draw_qkv(rng_key, lead_dims):
    col_gain = jnp.concatenate([jnp.full((WIDTH,), Q_GAIN, jnp.float32), jnp.ones((2 * WIDTH,), jnp.float32)])
    raw_vals = jax.random.normal(rng_key, lead_dims + (WIDTH, 3 * WIDTH), jnp.float32)
    return (raw_vals * col_gain * WIDTH ** -0.5).astype(jnp.bfloat16)


def draw_norms(rng_key, lead_dims, row_count):
    centre = jnp.tile(jnp.array([1.0, 0.0], jnp.float32), row_count // 2)[:, None]
    raw_vals = jax.random.normal(rng_key, lead_dims + (row_count, WIDTH), jnp.float32)
    return (raw_vals * 0.2 + centre).astype(jnp.bfloat16)


def setup_inputs(seed: int = 0, part: int = 0) -> dict:
    part_keys = jax.random.split(jax.random.fold_in(jax.random.key(seed), part), 2)
    rng_keys = jax.random.split(jax.random.key(seed + 1), 15)
    in_lead = (2, IN_BLOCKS)
    out_lead = (LAYERS,)
    return {
        "latents": draw_normal(part_keys[0], (TOKENS, WIDTH), 1.0),
        "hint_embed": draw_normal(part_keys[1], (TOKENS, WIDTH), 1.0),
        "in_qkv": draw_qkv(rng_keys[0], in_lead),
        "in_proj": draw_normal(rng_keys[1], in_lead + (HEADS, HEAD_DIM, WIDTH), WIDTH ** -0.5),
        "in_up": draw_normal(rng_keys[2], in_lead + (WIDTH, 4 * WIDTH), WIDTH ** -0.5),
        "in_down": draw_normal(rng_keys[3], in_lead + (4 * WIDTH, WIDTH), (4 * WIDTH) ** -0.5),
        "in_norm": draw_norms(rng_keys[4], in_lead, 4),
        "out_qkv": draw_qkv(rng_keys[5], out_lead),
        "out_proj": draw_normal(rng_keys[6], out_lead + (HEADS, HEAD_DIM, WIDTH), WIDTH ** -0.5),
        "out_up": draw_normal(rng_keys[7], out_lead + (WIDTH, 4 * WIDTH), WIDTH ** -0.5),
        "out_down": draw_normal(rng_keys[8], out_lead + (4 * WIDTH, WIDTH), (4 * WIDTH) ** -0.5),
        "out_norm": draw_norms(rng_keys[9], out_lead, 4),
        "zero_proj": draw_normal(rng_keys[10], (IN_BLOCKS, WIDTH, WIDTH), 0.6 * WIDTH ** -0.5),
        "hint_proj": draw_normal(rng_keys[11], (WIDTH, WIDTH), WIDTH ** -0.5),
        "skip_proj": draw_normal(rng_keys[12], (LAYERS, 2 * WIDTH, WIDTH), (2 * WIDTH) ** -0.5),
        "final_norm": draw_norms(rng_keys[13], (), 2),
        "w_out": draw_normal(rng_keys[14], (WIDTH, WIDTH), WIDTH ** -0.5),
    }


def mat_f32(left_op, right_op):
    return jnp.dot(left_op, right_op, preferred_element_type=jnp.float32)


def layer_norm(values, norm_gain, norm_shift):
    wide_vals = values.astype(jnp.float32)
    centered = wide_vals - jnp.mean(wide_vals, axis=-1, keepdims=True)
    variance = jnp.mean(centered * centered, axis=-1, keepdims=True)
    normed = centered * lax.rsqrt(variance + EPS)
    return (normed * norm_gain.astype(jnp.float32) + norm_shift.astype(jnp.float32)).astype(jnp.bfloat16)


def head_attend(head_args):
    queries, key_rows, val_rows = head_args
    scores = mat_f32(queries, key_rows.T) * HEAD_DIM ** -0.5
    att_probs = jax.nn.softmax(scores, axis=-1).astype(jnp.bfloat16)
    return mat_f32(att_probs, val_rows).astype(jnp.bfloat16)


def transformer_block(residual, params):
    w_qkv, w_proj, w_up, w_down, norm_rows = params
    normed = layer_norm(residual, norm_rows[0], norm_rows[1])
    qkv_all = mat_f32(normed, w_qkv).astype(jnp.bfloat16)
    by_head = qkv_all.reshape(TOKENS, 3, HEADS, HEAD_DIM).transpose(1, 2, 0, 3)
    head_out = lax.map(head_attend, (by_head[0], by_head[1], by_head[2]))
    head_out = head_out.transpose(1, 0, 2).reshape(TOKENS, WIDTH)
    residual = (residual.astype(jnp.float32) + mat_f32(head_out, w_proj.reshape(WIDTH, WIDTH))).astype(jnp.bfloat16)
    normed = layer_norm(residual, norm_rows[2], norm_rows[3])
    hidden = jax.nn.gelu(mat_f32(normed, w_up), approximate=True).astype(jnp.bfloat16)
    return (residual.astype(jnp.float32) + mat_f32(hidden, w_down)).astype(jnp.bfloat16)


def reference(latents, hint_embed, in_qkv, in_proj, in_up, in_down, in_norm, out_qkv, out_proj, out_up, out_down, out_norm, zero_proj, hint_proj, skip_proj, final_norm, w_out):
    def in_step(residual, params):
        residual = transformer_block(residual, params)
        return residual, residual

    def out_step(residual, xs_pack):
        merged = mat_f32(jnp.concatenate([residual, xs_pack[6]], axis=-1), xs_pack[5]).astype(jnp.bfloat16)
        return transformer_block(merged, xs_pack[:5]), None

    ctrl_start = (latents.astype(jnp.float32) + mat_f32(hint_embed, hint_proj)).astype(jnp.bfloat16)
    base_params = (in_qkv[0], in_proj[0], in_up[0], in_down[0], in_norm[0])
    ctrl_params = (in_qkv[1], in_proj[1], in_up[1], in_down[1], in_norm[1])
    base_outs = lax.scan(in_step, latents, base_params)[1]
    ctrl_outs = lax.scan(in_step, ctrl_start, ctrl_params)[1]
    ctrl_res = jnp.einsum("bnd,bde->bne", ctrl_outs.astype(jnp.float32), zero_proj.astype(jnp.float32)).astype(jnp.bfloat16)
    sum_all = (base_outs.astype(jnp.float32) + ctrl_res.astype(jnp.float32)).astype(jnp.bfloat16)
    out_xs = (out_qkv, out_proj, out_up, out_down, out_norm, skip_proj, sum_all[:LAYERS][::-1])
    out_state = lax.scan(out_step, sum_all[LAYERS], out_xs)[0]
    normed = layer_norm(out_state, final_norm[0], final_norm[1])
    return mat_f32(normed, w_out).astype(jnp.bfloat16)
```

```python
import functools
import jax
import jax.numpy as jnp
from jax import lax
from jax.experimental import pallas as pl
from jax.experimental.pallas import tpu as pltpu
from jax.sharding import PartitionSpec as P

EPS = 1e-6
LOG2E = 1.4426950408889634
F32 = jnp.float32
BF16 = jnp.bfloat16
VMEM_LIMIT = 60 * 1024 * 1024


def mat_f32(left_op, right_op):
    return jnp.dot(left_op, right_op, preferred_element_type=F32)


def layer_norm(values, norm_gain, norm_shift):
    wide_vals = values.astype(F32)
    centered = wide_vals - jnp.mean(wide_vals, axis=-1, keepdims=True)
    variance = jnp.mean(centered * centered, axis=-1, keepdims=True)
    normed = centered * lax.rsqrt(variance + EPS)
    return (normed * norm_gain.astype(F32) + norm_shift.astype(F32)).astype(BF16)


def qkv_kernel(br_ref, u_ref, norm_ref, w_ref, out_ref, t_ref, *, heads, head_dim):
    @pl.when(pl.program_id(0) == 0)
    def _():
        t_ref[...] = layer_norm(u_ref[...], norm_ref[0, 0, 0:1, :], norm_ref[0, 0, 1:2, :])

    prod = mat_f32(t_ref[...], w_ref[0, 0]).T
    tokens = prod.shape[1]
    out_ref[...] = prod.reshape(heads, 1, head_dim, tokens).astype(BF16)


def qkv_call(branch, layer, u, norm, w_qkv, heads):
    tokens, width = u.shape
    head_dim = width // heads
    grid_spec = pltpu.PrefetchScalarGridSpec(
        num_scalar_prefetch=1,
        grid=(3,),
        in_specs=[
            pl.BlockSpec((tokens, width), lambda n, br: (0, 0)),
            pl.BlockSpec((1, 1, 4, width), lambda n, br: (br[0], layer, 0, 0)),
            pl.BlockSpec((1, 1, width, width), lambda n, br: (br[0], layer, 0, n)),
        ],
        out_specs=pl.BlockSpec((heads, 1, head_dim, tokens), lambda n, br: (0, n, 0, 0)),
        scratch_shapes=[pltpu.VMEM((tokens, width), BF16)],
    )
    return pl.pallas_call(
        functools.partial(qkv_kernel, heads=heads, head_dim=head_dim),
        grid_spec=grid_spec,
        out_shape=jax.ShapeDtypeStruct((heads, 3, head_dim, tokens), BF16),
        compiler_params=pltpu.CompilerParams(vmem_limit_bytes=VMEM_LIMIT, dimension_semantics=("arbitrary",)),
        cost_estimate=pl.CostEstimate(flops=6 * tokens * width * width, bytes_accessed=6 * width * width, transcendentals=0),
        name="ln_qkv",
    )(branch, u, norm, w_qkv)


def post_kernel(br_ref, at_ref, u_ref, norm_ref, wo_ref, w1_ref, w2_ref, out_ref, res_ref, t_ref, acc_ref):
    step = pl.program_id(0)

    @pl.when(step == 0)
    def _():
        att = at_ref[...].T
        res = (u_ref[...].astype(F32) + mat_f32(att, wo_ref[0, 0])).astype(BF16)
        res_ref[...] = res
        t_ref[...] = layer_norm(res, norm_ref[0, 0, 2:3, :], norm_ref[0, 0, 3:4, :])

    hidden = jax.nn.gelu(mat_f32(t_ref[...], w1_ref[0, 0]), approximate=True).astype(BF16)
    part = mat_f32(hidden, w2_ref[0, 0])

    @pl.when(step == 0)
    def _():
        acc_ref[...] = part

    @pl.when(step > 0)
    def _():
        acc_ref[...] += part

    @pl.when(step == pl.num_programs(0) - 1)
    def _():
        out_ref[...] = (res_ref[...].astype(F32) + acc_ref[...]).astype(BF16)


def post_call(branch, layer, att_t, u, norm, w_proj, w_up, w_down):
    tokens, width = u.shape
    hidden = w_up.shape[-1]
    tile = hidden // 6
    grid_spec = pltpu.PrefetchScalarGridSpec(
        num_scalar_prefetch=1,
        grid=(6,),
        in_specs=[
            pl.BlockSpec((width, tokens), lambda n, br: (0, 0)),
            pl.BlockSpec((tokens, width), lambda n, br: (0, 0)),
            pl.BlockSpec((1, 1, 4, width), lambda n, br: (br[0], layer, 0, 0)),
            pl.BlockSpec((1, 1, width, width), lambda n, br: (br[0], layer, 0, 0)),
            pl.BlockSpec((1, 1, width, tile), lambda n, br: (br[0], layer, 0, n)),
            pl.BlockSpec((1, 1, tile, width), lambda n, br: (br[0], layer, n, 0)),
        ],
        out_specs=pl.BlockSpec((tokens, width), lambda n, br: (0, 0)),
        scratch_shapes=[
            pltpu.VMEM((tokens, width), BF16),
            pltpu.VMEM((tokens, width), BF16),
            pltpu.VMEM((tokens, width), F32),
        ],
    )
    return pl.pallas_call(
        post_kernel,
        grid_spec=grid_spec,
        out_shape=jax.ShapeDtypeStruct((tokens, width), BF16),
        compiler_params=pltpu.CompilerParams(vmem_limit_bytes=VMEM_LIMIT, dimension_semantics=("arbitrary",)),
        cost_estimate=pl.CostEstimate(
            flops=2 * tokens * width * (width + 2 * hidden), bytes_accessed=2 * width * (width + 2 * hidden), transcendentals=tokens * hidden
        ),
        name="proj_mlp",
    )(branch, att_t, u, norm, w_proj, w_up, w_down)


def attn_kernel(q_ref, kv_ref, out_ref, q2_ref, k2_ref, v_ref, s_ref, *, scale, chunk, q_tile):
    q_src, head_dim, span = q_ref.shape
    srcs = kv_ref.shape[0]
    keys = srcs * span
    per_q = q_tile // span
    q_tiles = q_src // per_q
    chunks = keys // chunk
    per_chunk = chunk // span
    v_rows = v_ref.shape[1]
    ones_row = (lax.broadcasted_iota(jnp.int32, (v_rows - head_dim, span), 0) == 0).astype(F32)

    def fill_kv(src, carry):
        key_t = kv_ref[src, 0].astype(F32)
        two_keys = jnp.concatenate([key_t, key_t], axis=0)
        k2_ref[pl.ds(pl.multiple_of(src * span, span), span), :] = two_keys.T.astype(BF16)
        val_t = jnp.concatenate([kv_ref[src, 1].astype(F32), ones_row], axis=0).astype(BF16)
        lane = pl.multiple_of(lax.rem(src, per_chunk) * span, span)
        v_ref[src // per_chunk, :, pl.ds(lane, span)] = val_t
        return carry

    lax.fori_loop(0, srcs, fill_kv, 0)

    def fill_q(src, carry):
        wide = q_ref[src].astype(F32) * (scale * LOG2E)
        high = wide.astype(BF16)
        low = (wide - high.astype(F32)).astype(F32)
        both = jnp.concatenate([high.astype(F32), low], axis=0).astype(BF16)
        lane = pl.multiple_of(lax.rem(src, per_q) * span, span)
        q2_ref[src // per_q, :, pl.ds(lane, span)] = both
        return carry

    lax.fori_loop(0, q_src, fill_q, 0)

    def score_chunk(tile, slot, idx, peak):
        part = mat_f32(k2_ref[idx * chunk:(idx + 1) * chunk, :], q2_ref[tile])
        s_ref[slot, idx * chunk:(idx + 1) * chunk, :] = part
        return jnp.maximum(peak, jnp.max(part.reshape(chunk // 8, 8, q_tile), axis=0))

    low_peak = jnp.full((8, q_tile), -jnp.inf, F32)
    peak = low_peak
    for idx in range(chunks):
        peak = score_chunk(0, 0, idx, peak)

    def one_tile(tile, peak):
        slot = lax.rem(tile, 2)
        nxt = jnp.minimum(tile + 1, q_tiles - 1)
        top = jnp.max(peak, axis=0, keepdims=True)
        acc = jnp.zeros((v_rows, q_tile), F32)
        new_peak = low_peak
        for idx in range(chunks):
            new_peak = score_chunk(nxt, 1 - slot, idx, new_peak)
            probs = jnp.exp2(s_ref[slot, idx * chunk:(idx + 1) * chunk, :] - top).astype(BF16)
            acc = acc + mat_f32(v_ref[idx], probs)
        normed = (acc[:head_dim] / acc[head_dim:head_dim + 1]).astype(BF16)
        for sub in range(per_q):
            out_ref[tile * per_q + sub] = normed[:, sub * span:(sub + 1) * span]
        return new_peak

    lax.fori_loop(0, q_tiles, one_tile, peak)


def attn_call(q_t, kv_t, chunk=512, q_tile=256):
    q_src, head_dim, span = q_t.shape
    srcs = kv_t.shape[0]
    keys = srcs * span
    v_rows = head_dim + 8
    return pl.pallas_call(
        functools.partial(attn_kernel, scale=head_dim ** -0.5, chunk=chunk, q_tile=q_tile),
        in_specs=[pl.BlockSpec(memory_space=pltpu.VMEM)] * 2,
        out_specs=pl.BlockSpec(memory_space=pltpu.VMEM),
        out_shape=jax.ShapeDtypeStruct((q_src, head_dim, span), BF16),
        scratch_shapes=[
            pltpu.VMEM((q_src * span // q_tile, 2 * head_dim, q_tile), BF16),
            pltpu.VMEM((keys, 2 * head_dim), BF16),
            pltpu.VMEM((keys // chunk, v_rows, chunk), BF16),
            pltpu.VMEM((2, keys, q_tile), F32),
        ],
        compiler_params=pltpu.CompilerParams(vmem_limit_bytes=VMEM_LIMIT),
        cost_estimate=pl.CostEstimate(
            flops=4 * q_src * span * keys * head_dim, bytes_accessed=4 * keys * head_dim * 4, transcendentals=q_src * span * keys
        ),
        name="attention",
    )(q_t, kv_t)


def barrier_all(peers):
    sem = pltpu.get_barrier_semaphore()
    for peer in peers:
        pl.semaphore_signal(sem, inc=1, device_id={"group": peer}, device_id_type=pl.DeviceIdType.MESH)
    pl.semaphore_wait(sem, len(peers))


def plane_exchange_kernel(x_ref, out_ref, send_sem, recv_sem, own_sem):
    chips = x_ref.shape[0]
    me = lax.axis_index("group")
    chip, core = me // 2, lax.rem(me, 2)
    others = [lax.rem(chip + off, chips) for off in range(1, chips)]
    barrier_all([2 * other + core for other in others])
    own = pltpu.make_async_copy(x_ref.at[chip], out_ref.at[chip], own_sem)
    own.start()
    copies = []
    for off, other in enumerate(others):
        copy = pltpu.make_async_remote_copy(
            src_ref=x_ref.at[other],
            dst_ref=out_ref.at[chip],
            send_sem=send_sem.at[off],
            recv_sem=recv_sem.at[off],
            device_id={"group": 2 * other + core},
            device_id_type=pl.DeviceIdType.MESH,
        )
        copy.start()
        copies.append(copy)
    own.wait()
    for copy in copies:
        copy.wait()


def plane_exchange(x, collective_id):
    chips = x.shape[0]
    return pl.pallas_call(
        plane_exchange_kernel,
        in_specs=[pl.BlockSpec(memory_space=pltpu.VMEM)],
        out_specs=pl.BlockSpec(memory_space=pltpu.VMEM),
        out_shape=jax.ShapeDtypeStruct(x.shape, x.dtype),
        scratch_shapes=[pltpu.SemaphoreType.DMA((chips - 1,)), pltpu.SemaphoreType.DMA((chips - 1,)), pltpu.SemaphoreType.DMA],
        compiler_params=pltpu.CompilerParams(collective_id=collective_id, has_side_effects=True, vmem_limit_bytes=VMEM_LIMIT),
        name="plane_exchange",
    )(x)


def spread_kernel(q_ref, kv_ref, q_out, kv_out, send_sem, recv_sem, own_sem):
    chips = q_ref.shape[0]
    group = 2 * chips
    me = lax.axis_index("group")
    chip, core = me // 2, lax.rem(me, 2)
    barrier_all([lax.rem(me + off, group) for off in range(1, group)])
    own = [
        pltpu.make_async_copy(q_ref.at[chip], q_out.at[chip], own_sem.at[0]),
        pltpu.make_async_copy(kv_ref.at[chip], kv_out.at[me], own_sem.at[1]),
    ]
    for copy in own:
        copy.start()
    copies = []
    for off in range(1, group):
        peer = lax.rem(me + off, group)
        copies.append(pltpu.make_async_remote_copy(
            src_ref=kv_ref.at[peer // 2], dst_ref=kv_out.at[me], send_sem=send_sem.at[off], recv_sem=recv_sem.at[off],
            device_id={"group": peer}, device_id_type=pl.DeviceIdType.MESH))
        copies[-1].start()
    for off in range(1, chips):
        other = lax.rem(chip + off, chips)
        copies.append(pltpu.make_async_remote_copy(
            src_ref=q_ref.at[other], dst_ref=q_out.at[chip], send_sem=send_sem.at[group + off], recv_sem=recv_sem.at[group + off],
            device_id={"group": 2 * other + core}, device_id_type=pl.DeviceIdType.MESH))
        copies[-1].start()
    for copy in own:
        copy.wait()
    for copy in copies:
        copy.wait()


def spread(q_t, kv_t, collective_id):
    chips = q_t.shape[0]
    sems = 3 * chips
    return pl.pallas_call(
        spread_kernel,
        in_specs=[pl.BlockSpec(memory_space=pltpu.VMEM)] * 2,
        out_specs=[pl.BlockSpec(memory_space=pltpu.VMEM)] * 2,
        out_shape=[jax.ShapeDtypeStruct(q_t.shape, q_t.dtype), jax.ShapeDtypeStruct((2 * chips,) + kv_t.shape[1:], kv_t.dtype)],
        scratch_shapes=[pltpu.SemaphoreType.DMA((sems,)), pltpu.SemaphoreType.DMA((sems,)), pltpu.SemaphoreType.DMA((2,))],
        compiler_params=pltpu.CompilerParams(collective_id=collective_id, has_side_effects=True, vmem_limit_bytes=VMEM_LIMIT),
        name="spread",
    )(q_t, kv_t)


def solution(mesh):
    group_size = mesh.shape["group"]
    chips = group_size // 2
    swap = [(dev, dev ^ 1) for dev in range(group_size)]

    def device_step(x_own, hint_own, in_qkv, in_proj, in_up, in_down, in_norm, out_qkv, out_proj, out_up, out_down, out_norm, zero_proj, hint_proj, skip_proj, final_norm, w_out):
        layers = skip_proj.shape[0]
        tok_own, width = x_own.shape
        heads = in_proj.shape[2]
        head_dim = width // heads
        me = lax.axis_index("group")
        is_base = me % 2 == 0
        branch = jnp.reshape((me % 2).astype(jnp.int32), (1,))
        zero = jnp.zeros((1,), jnp.int32)
        in_proj = in_proj.reshape(in_proj.shape[:2] + (width, width))
        out_proj = out_proj.reshape((1, layers, width, width))
        out_qkv, out_up, out_down, out_norm = out_qkv[None], out_up[None], out_down[None], out_norm[None]

        both = jnp.concatenate([x_own, hint_own], axis=0)
        both_other = lax.ppermute(both, "group", swap)
        x_other, hint_other = both_other[:tok_own], both_other[tok_own:]
        x_local = jnp.where(is_base, jnp.concatenate([x_own, x_other], axis=0), jnp.concatenate([x_other, x_own], axis=0))
        hint_local = jnp.where(is_base, jnp.zeros((2 * tok_own, width), BF16), jnp.concatenate([hint_other, hint_own], axis=0))
        state = (x_local.astype(F32) + mat_f32(hint_local, hint_proj)).astype(BF16)
        sums = []
        for layer in range(layers + 1):
            qkv_t = qkv_call(branch, layer, state, in_norm, in_qkv, heads)
            moved = plane_exchange(qkv_t, 0)
            att_t = attn_call(moved[:, 0], moved[:, 1:])
            back = plane_exchange(att_t, 1).reshape(width, 2 * tok_own)
            state = post_call(branch, layer, back, state, in_norm, in_proj, in_up, in_down)
            ctrl_res = mat_f32(state, zero_proj[layer]).astype(BF16)
            give = jnp.where(is_base, state[tok_own:], ctrl_res[:tok_own])
            keep = jnp.where(is_base, state[:tok_own], ctrl_res[tok_own:])
            got = lax.ppermute(give, "group", swap)
            sums.append((keep.astype(F32) + got.astype(F32)).astype(BF16))
        out_state = sums.pop()
        for layer in range(layers):
            skip_val = sums[layers - 1 - layer]
            merged = (mat_f32(out_state, skip_proj[layer, :width]) + mat_f32(skip_val, skip_proj[layer, width:])).astype(BF16)
            qkv_t = qkv_call(zero, layer, merged, out_norm, out_qkv, heads)
            q_moved, kv_moved = spread(qkv_t[:, 0], qkv_t[:, 1:], 2)
            att_t = attn_call(q_moved, kv_moved)
            back = plane_exchange(att_t, 3).reshape(width, tok_own)
            out_state = post_call(zero, layer, back, merged, out_norm, out_proj, out_up, out_down)
        normed = layer_norm(out_state, final_norm[0], final_norm[1])
        return mat_f32(normed, w_out).astype(BF16)

    tok_spec = P(("data", "group"), None)
    return jax.shard_map(device_step, mesh=mesh, in_specs=(tok_spec, tok_spec) + (P(),) * 15, out_specs=tok_spec, check_vma=False)
```

```python
import functools
import jax
import jax.numpy as jnp
from jax import lax
from jax.experimental import pallas as pl
from jax.experimental.pallas import tpu as pltpu
from jax.sharding import PartitionSpec as P

EPS = 1e-6
LOG2E = 1.4426950408889634
F32 = jnp.float32
BF16 = jnp.bfloat16
VMEM_LIMIT = 60 * 1024 * 1024


def mat_f32(left_op, right_op):
    return jnp.dot(left_op, right_op, preferred_element_type=F32)


def layer_norm(values, norm_gain, norm_shift):
    wide_vals = values.astype(F32)
    centered = wide_vals - jnp.mean(wide_vals, axis=-1, keepdims=True)
    variance = jnp.mean(centered * centered, axis=-1, keepdims=True)
    normed = centered * lax.rsqrt(variance + EPS)
    return (normed * norm_gain.astype(F32) + norm_shift.astype(F32)).astype(BF16)


def qkv_kernel(br_ref, u_ref, norm_ref, w_ref, out_ref, t_ref, *, heads, head_dim):
    @pl.when(pl.program_id(0) == 0)
    def _():
        t_ref[...] = layer_norm(u_ref[...], norm_ref[0, 0, 0:1, :], norm_ref[0, 0, 1:2, :])

    prod = mat_f32(t_ref[...], w_ref[0, 0]).T
    tokens = prod.shape[1]
    out_ref[...] = prod.reshape(heads, 1, head_dim, tokens).astype(BF16)


def qkv_call(branch, layer, u, norm, w_qkv, heads):
    tokens, width = u.shape
    head_dim = width // heads
    grid_spec = pltpu.PrefetchScalarGridSpec(
        num_scalar_prefetch=1,
        grid=(3,),
        in_specs=[
            pl.BlockSpec((tokens, width), lambda n, br: (0, 0)),
            pl.BlockSpec((1, 1, 4, width), lambda n, br: (br[0], layer, 0, 0)),
            pl.BlockSpec((1, 1, width, width), lambda n, br: (br[0], layer, 0, n)),
        ],
        out_specs=pl.BlockSpec((heads, 1, head_dim, tokens), lambda n, br: (0, n, 0, 0)),
        scratch_shapes=[pltpu.VMEM((tokens, width), BF16)],
    )
    return pl.pallas_call(
        functools.partial(qkv_kernel, heads=heads, head_dim=head_dim),
        grid_spec=grid_spec,
        out_shape=jax.ShapeDtypeStruct((heads, 3, head_dim, tokens), BF16),
        compiler_params=pltpu.CompilerParams(vmem_limit_bytes=VMEM_LIMIT, dimension_semantics=("arbitrary",)),
        cost_estimate=pl.CostEstimate(flops=6 * tokens * width * width, bytes_accessed=6 * width * width, transcendentals=0),
        name="ln_qkv",
    )(branch, u, norm, w_qkv)


def post_kernel(br_ref, at_ref, u_ref, norm_ref, wo_ref, w1_ref, w2_ref, out_ref, res_ref, t_ref, acc_ref):
    step = pl.program_id(0)

    @pl.when(step == 0)
    def _():
        att = at_ref[...].T
        res = (u_ref[...].astype(F32) + mat_f32(att, wo_ref[0, 0])).astype(BF16)
        res_ref[...] = res
        t_ref[...] = layer_norm(res, norm_ref[0, 0, 2:3, :], norm_ref[0, 0, 3:4, :])

    hidden = jax.nn.gelu(mat_f32(t_ref[...], w1_ref[0, 0]), approximate=True).astype(BF16)
    part = mat_f32(hidden, w2_ref[0, 0])

    @pl.when(step == 0)
    def _():
        acc_ref[...] = part

    @pl.when(step > 0)
    def _():
        acc_ref[...] += part

    @pl.when(step == pl.num_programs(0) - 1)
    def _():
        out_ref[...] = (res_ref[...].astype(F32) + acc_ref[...]).astype(BF16)


def post_call(branch, layer, att_t, u, norm, w_proj, w_up, w_down):
    tokens, width = u.shape
    hidden = w_up.shape[-1]
    tile = hidden // 6
    grid_spec = pltpu.PrefetchScalarGridSpec(
        num_scalar_prefetch=1,
        grid=(6,),
        in_specs=[
            pl.BlockSpec((width, tokens), lambda n, br: (0, 0)),
            pl.BlockSpec((tokens, width), lambda n, br: (0, 0)),
            pl.BlockSpec((1, 1, 4, width), lambda n, br: (br[0], layer, 0, 0)),
            pl.BlockSpec((1, 1, width, width), lambda n, br: (br[0], layer, 0, 0)),
            pl.BlockSpec((1, 1, width, tile), lambda n, br: (br[0], layer, 0, n)),
            pl.BlockSpec((1, 1, tile, width), lambda n, br: (br[0], layer, n, 0)),
        ],
        out_specs=pl.BlockSpec((tokens, width), lambda n, br: (0, 0)),
        scratch_shapes=[
            pltpu.VMEM((tokens, width), BF16),
            pltpu.VMEM((tokens, width), BF16),
            pltpu.VMEM((tokens, width), F32),
        ],
    )
    return pl.pallas_call(
        post_kernel,
        grid_spec=grid_spec,
        out_shape=jax.ShapeDtypeStruct((tokens, width), BF16),
        compiler_params=pltpu.CompilerParams(vmem_limit_bytes=VMEM_LIMIT, dimension_semantics=("arbitrary",)),
        cost_estimate=pl.CostEstimate(
            flops=2 * tokens * width * (width + 2 * hidden), bytes_accessed=2 * width * (width + 2 * hidden), transcendentals=tokens * hidden
        ),
        name="proj_mlp",
    )(branch, att_t, u, norm, w_proj, w_up, w_down)


def attend_kernel(x_ref, back_ref, q_in, kv_in, o_buf, q2a_ref, q2b_ref, k2_ref, v_ref, sa_ref, sb_ref,
                  q_send, q_recv, kv_send, kv_recv, o_send, o_recv, sib_send, sib_recv, own_sem, *, scale, chunk, q_tile, share):
    chips, _, head_dim, span = x_ref.shape
    me = lax.axis_index("group")
    chip, core = me // 2, lax.rem(me, 2)
    sibling = me + 1 - 2 * core
    per_q = q_tile // span
    q_tiles = chips // per_q
    chunks = k2_ref.shape[0] // chunk
    per_chunk = chunk // span
    v_rows = v_ref.shape[1]

    def ahead(off):
        return lax.rem(chip + off, chips)

    def behind(off):
        return lax.rem(chip + chips - off, chips)

    def to_device(src, dst, send, recv, device):
        return pltpu.make_async_remote_copy(
            src_ref=src, dst_ref=dst, send_sem=send, recv_sem=recv, device_id={"group": device}, device_id_type=pl.DeviceIdType.MESH)

    def q_copy(off):
        return to_device(x_ref.at[ahead(off), 0], q_in.at[off], q_send.at[off], q_recv.at[off], 2 * ahead(off) + core)

    def kv_copy(off):
        return to_device(x_ref.at[ahead(off), pl.ds(1, 2)], kv_in.at[off], kv_send.at[off], kv_recv.at[off], 2 * ahead(off) + core)

    def o_copy(off):
        return to_device(o_buf.at[off], back_ref.at[chip], o_send.at[off], o_recv.at[off], 2 * behind(off) + core)

    def sib_copy(off):
        return to_device(kv_in.at[off], kv_in.at[chips + off], sib_send.at[off], sib_recv.at[off], sibling)

    sem = pltpu.get_barrier_semaphore()
    greeted = [2 * ahead(off) + core for off in range(1, chips)] + ([sibling] if share else [])
    for peer in greeted:
        pl.semaphore_signal(sem, inc=1, device_id={"group": peer}, device_id_type=pl.DeviceIdType.MESH)
    own_q = pltpu.make_async_copy(x_ref.at[chip, 0], q_in.at[0], own_sem.at[0])
    own_kv = pltpu.make_async_copy(x_ref.at[chip, pl.ds(1, 2)], kv_in.at[0], own_sem.at[1])
    own_o = pltpu.make_async_copy(o_buf.at[0], back_ref.at[chip], own_sem.at[2])
    own_q.start()
    own_kv.start()
    pl.semaphore_wait(sem, len(greeted))
    for off in range(1, per_q):
        q_copy(off).start()
    for off in range(1, chips):
        kv_copy(off).start()
    for off in range(per_q, chips):
        q_copy(off).start()

    ones_row = (lax.broadcasted_iota(jnp.int32, (v_rows - head_dim, span), 0) == 0).astype(F32)
    low_peak = jnp.full((8, q_tile), -jnp.inf, F32)

    def fill_q(dst, src, part):
        wide = q_in[src].astype(F32) * (scale * LOG2E)
        high = wide.astype(BF16).astype(F32)
        dst[:, part * span:(part + 1) * span] = jnp.concatenate([high, wide - high], axis=0).astype(BF16)

    def score(dst, rows, q2, peak):
        part = mat_f32(k2_ref[rows, :], q2)
        dst[rows, :] = part
        return jnp.maximum(peak, jnp.max(part.reshape(part.shape[0] // 8, 8, q_tile), axis=0))

    def take_kv(src, peak):
        key_t = kv_in[src, 0].astype(F32)
        rows = pl.ds(pl.multiple_of(src * span, span), span)
        k2_ref[rows, :] = jnp.concatenate([key_t, key_t], axis=0).T.astype(BF16)
        val_t = jnp.concatenate([kv_in[src, 1].astype(F32), ones_row], axis=0).astype(BF16)
        v_ref[src // per_chunk, :, pl.ds(pl.multiple_of(lax.rem(src, per_chunk) * span, span), span)] = val_t
        return score(sa_ref, rows, q2a_ref[...], peak)

    own_q.wait()
    own_kv.wait()
    fill_q(q2a_ref, 0, 0)
    for off in range(1, per_q):
        q_copy(off).wait_recv()
        fill_q(q2a_ref, off, off)
    if share:
        sib_copy(0).start()
    peak = take_kv(0, low_peak)

    def arrive(off, peak):
        kv_copy(off).wait_recv()
        if share:
            sib_copy(off).start()
        return take_kv(off, peak)

    peak = lax.fori_loop(1, chips, arrive, peak)
    if share:
        def arrive_sib(off, peak):
            sib_copy(off).wait_recv()
            return take_kv(chips + off, peak)

        peak = lax.fori_loop(0, chips, arrive_sib, peak)

    def one_tile(tile, q2_ref, cur_ref, nxt_ref, peak):
        @pl.when(tile > 1)
        def _():
            for sub in range(per_q):
                o_copy((tile - 1) * per_q + sub).start()

        @pl.when(tile < q_tiles - 1)
        def _():
            for sub in range(per_q):
                off = (tile + 1) * per_q + sub
                q_copy(off).wait_recv()
                fill_q(q2_ref, off, sub)

        top = jnp.max(peak, axis=0, keepdims=True)
        acc = jnp.zeros((v_rows, q_tile), F32)
        new_peak = low_peak
        q2 = q2_ref[...]
        for idx in range(chunks):
            rows = slice(idx * chunk, (idx + 1) * chunk)
            new_peak = score(nxt_ref, rows, q2, new_peak)
            probs = jnp.exp2(cur_ref[rows, :] - top).astype(BF16)
            acc = acc + mat_f32(v_ref[idx], probs)
        normed = (acc[:head_dim] / acc[head_dim:head_dim + 1]).astype(BF16)
        for sub in range(per_q):
            o_buf[tile * per_q + sub] = normed[:, sub * span:(sub + 1) * span]
        return new_peak

    def two_tiles(pair, peak):
        peak = one_tile(2 * pair, q2b_ref, sa_ref, sb_ref, peak)
        return one_tile(2 * pair + 1, q2a_ref, sb_ref, sa_ref, peak)

    lax.fori_loop(0, q_tiles // 2, two_tiles, peak)
    own_o.start()
    for off in range(1, per_q):
        o_copy(off).start()
    for off in range(chips - per_q, chips):
        o_copy(off).start()
    own_o.wait()

    def finish(off, carry):
        q_copy(off).wait_send()
        kv_copy(off).wait_send()
        o_copy(off).wait_send()
        o_copy(off).wait_recv()
        return carry

    lax.fori_loop(1, chips, finish, 0)
    if share:
        def finish_sib(off, carry):
            sib_copy(off).wait_send()
            return carry

        lax.fori_loop(0, chips, finish_sib, 0)


def attend(x, collective_id, share, chunk=512, q_tile=256):
    chips, _, head_dim, span = x.shape
    srcs = 2 * chips if share else chips
    keys = srcs * span
    v_rows = head_dim + 8
    dma = pltpu.SemaphoreType.DMA
    return pl.pallas_call(
        functools.partial(attend_kernel, scale=head_dim ** -0.5, chunk=chunk, q_tile=q_tile, share=share),
        in_specs=[pl.BlockSpec(memory_space=pl.ANY)],
        out_specs=pl.BlockSpec(memory_space=pltpu.VMEM),
        out_shape=jax.ShapeDtypeStruct((chips, head_dim, span), BF16),
        scratch_shapes=[
            pltpu.VMEM((chips, head_dim, span), BF16),
            pltpu.VMEM((srcs, 2, head_dim, span), BF16),
            pltpu.VMEM((chips, head_dim, span), BF16),
            pltpu.VMEM((2 * head_dim, q_tile), BF16),
            pltpu.VMEM((2 * head_dim, q_tile), BF16),
            pltpu.VMEM((keys, 2 * head_dim), BF16),
            pltpu.VMEM((keys // chunk, v_rows, chunk), BF16),
            pltpu.VMEM((keys, q_tile), F32),
            pltpu.VMEM((keys, q_tile), F32),
        ] + [dma((chips,))] * 8 + [dma((3,))],
        compiler_params=pltpu.CompilerParams(collective_id=collective_id, has_side_effects=True, vmem_limit_bytes=VMEM_LIMIT),
        cost_estimate=pl.CostEstimate(
            flops=4 * chips * span * keys * head_dim, bytes_accessed=8 * keys * head_dim, transcendentals=chips * span * keys),
        name="attend",
    )(x)


def solution(mesh):
    group_size = mesh.shape["group"]
    chips = group_size // 2
    swap = [(dev, dev ^ 1) for dev in range(group_size)]

    def device_step(x_own, hint_own, in_qkv, in_proj, in_up, in_down, in_norm, out_qkv, out_proj, out_up, out_down, out_norm, zero_proj, hint_proj, skip_proj, final_norm, w_out):
        layers = skip_proj.shape[0]
        tok_own, width = x_own.shape
        heads = in_proj.shape[2]
        head_dim = width // heads
        me = lax.axis_index("group")
        is_base = me % 2 == 0
        branch = jnp.reshape((me % 2).astype(jnp.int32), (1,))
        zero = jnp.zeros((1,), jnp.int32)
        in_proj = in_proj.reshape(in_proj.shape[:2] + (width, width))
        out_proj = out_proj.reshape((1, layers, width, width))
        out_qkv, out_up, out_down, out_norm = out_qkv[None], out_up[None], out_down[None], out_norm[None]

        both = jnp.concatenate([x_own, hint_own], axis=0)
        both_other = lax.ppermute(both, "group", swap)
        x_other, hint_other = both_other[:tok_own], both_other[tok_own:]
        x_local = jnp.where(is_base, jnp.concatenate([x_own, x_other], axis=0), jnp.concatenate([x_other, x_own], axis=0))
        hint_local = jnp.where(is_base, jnp.zeros((2 * tok_own, width), BF16), jnp.concatenate([hint_other, hint_own], axis=0))
        state = (x_local.astype(F32) + mat_f32(hint_local, hint_proj)).astype(BF16)
        sums = []
        for layer in range(layers + 1):
            qkv_t = qkv_call(branch, layer, state, in_norm, in_qkv, heads)
            back = attend(qkv_t, 0, False).reshape(width, 2 * tok_own)
            state = post_call(branch, layer, back, state, in_norm, in_proj, in_up, in_down)
            ctrl_res = mat_f32(state, zero_proj[layer]).astype(BF16)
            give = jnp.where(is_base, state[tok_own:], ctrl_res[:tok_own])
            keep = jnp.where(is_base, state[:tok_own], ctrl_res[tok_own:])
            got = lax.ppermute(give, "group", swap)
            sums.append((keep.astype(F32) + got.astype(F32)).astype(BF16))
        out_state = sums.pop()
        for layer in range(layers):
            skip_val = sums[layers - 1 - layer]
            merged = (mat_f32(out_state, skip_proj[layer, :width]) + mat_f32(skip_val, skip_proj[layer, width:])).astype(BF16)
            qkv_t = qkv_call(zero, layer, merged, out_norm, out_qkv, heads)
            back = attend(qkv_t, 1, True).reshape(width, tok_own)
            out_state = post_call(zero, layer, back, merged, out_norm, out_proj, out_up, out_down)
        normed = layer_norm(out_state, final_norm[0], final_norm[1])
        return mat_f32(normed, w_out).astype(BF16)

    tok_spec = P(("data", "group"), None)
    return jax.shard_map(device_step, mesh=mesh, in_specs=(tok_spec, tok_spec) + (P(),) * 15, out_specs=tok_spec, check_vma=False)
```

```python
import functools
import jax
import jax.numpy as jnp
from jax import lax
from jax.experimental import pallas as pl
from jax.experimental.pallas import tpu as pltpu
from jax.sharding import PartitionSpec as P

EPS = 1e-6
LOG2E = 1.4426950408889634
F32 = jnp.float32
BF16 = jnp.bfloat16
VMEM_LIMIT = 67043328
MESH = pl.DeviceIdType.MESH


def mat_f32(left_op, right_op):
    return jnp.dot(left_op, right_op, preferred_element_type=F32)


def layer_norm(values, norm_gain, norm_shift):
    wide_vals = values.astype(F32)
    centered = wide_vals - jnp.mean(wide_vals, axis=-1, keepdims=True)
    variance = jnp.mean(centered * centered, axis=-1, keepdims=True)
    normed = centered * lax.rsqrt(variance + EPS)
    return (normed * norm_gain + norm_shift).astype(BF16)


def step_kernel(x_hbm, hint_hbm, in_qkv, in_proj, in_up, in_down, in_norm, out_qkv, out_proj, out_up, out_down, out_norm,
                zero_proj, hint_proj, skip_proj, final_norm, w_out, y_ref,
                wqkv_ref, wo_ref, w1_ref, w2_ref, ws_ref, u_ref, t_ref, acc_ref, x_buf, q_in, kv_in, o_buf, back_ref,
                q2a_ref, q2b_ref, k2_ref, v_ref, sa_ref, sb_ref, keep_ref, give_ref, got_ref,
                wqkv_sem, wo_sem, w1_sem, w2_sem, ws_sem, q_send, q_recv, kv_send, kv_recv, o_send, o_recv, sib_send, sib_recv,
                pair_send, pair_recv, own_sem, credit_sem, *, heads, chunk, q_tile):
    chips = heads
    width = u_ref.shape[1]
    head_dim = width // heads
    slab = x_hbm.shape[0]
    layers = skip_proj.shape[0]
    me = lax.axis_index("group")
    chip, core = me // 2, lax.rem(me, 2)
    sibling = me + 1 - 2 * core
    v_rows = v_ref.shape[1]
    chunks = k2_ref.shape[0] // chunk
    scale = head_dim ** -0.5 * LOG2E
    tile_w = width
    mlp_tiles = w1_ref.shape[1] // tile_w

    def ahead(off):
        return lax.rem(chip + off, chips)

    def behind(off):
        return lax.rem(chip + chips - off, chips)

    def to_device(src, dst, send, recv, device):
        return pltpu.make_async_remote_copy(
            src_ref=src, dst_ref=dst, send_sem=send, recv_sem=recv, device_id={"group": device}, device_id_type=MESH)

    def qkv_load(src, part):
        cols = pl.ds(part * width, width)
        return pltpu.make_async_copy(src.at[:, cols], wqkv_ref.at[:, cols], wqkv_sem.at[part])

    def square_load(src):
        return pltpu.make_async_copy(src, wo_ref, wo_sem)

    def up_load(src, part):
        cols = pl.ds(part * tile_w, tile_w)
        return pltpu.make_async_copy(src.at[:, cols], w1_ref.at[:, cols], w1_sem.at[part])

    def down_load(src, part):
        rows = pl.ds(part * tile_w, tile_w)
        return pltpu.make_async_copy(src.at[rows], w2_ref.at[rows], w2_sem.at[part])

    def skip_load(layer):
        return pltpu.make_async_copy(skip_proj.at[layer], ws_ref, ws_sem)

    def start_qkv(src):
        for part in (1, 2, 0):
            qkv_load(src, part).start()

    def start_mlp(up, down):
        for part in range(mlp_tiles):
            up_load(up, part).start()
            down_load(down, part).start()

    blocks = [(in_qkv.at[core, i], in_proj.at[core, i], in_up.at[core, i], in_down.at[core, i]) for i in range(layers + 1)]
    blocks += [(out_qkv.at[i], out_proj.at[i], out_up.at[i], out_down.at[i]) for i in range(layers)]

    sem = pltpu.get_barrier_semaphore()
    greeted = [2 * ahead(off) + core for off in range(1, chips)] + [sibling]
    for peer in greeted:
        pl.semaphore_signal(sem, inc=1, device_id={"group": peer}, device_id_type=MESH)
    mine = pl.ds(pl.multiple_of(core * slab, slab), slab)
    own_x = pltpu.make_async_copy(x_hbm, u_ref.at[mine], own_sem.at[0])
    own_h = pltpu.make_async_copy(hint_hbm, t_ref.at[mine], own_sem.at[1])
    own_x.start()
    own_h.start()
    square_load(hint_proj).start()
    start_qkv(blocks[0][0])
    start_mlp(blocks[0][2], blocks[0][3])
    pl.semaphore_wait(sem, len(greeted))
    sib_x = to_device(x_hbm, u_ref.at[mine], pair_send.at[0], pair_recv.at[0], sibling)
    sib_h = to_device(hint_hbm, t_ref.at[mine], pair_send.at[1], pair_recv.at[1], sibling)
    sib_x.start()
    sib_h.start()
    own_x.wait()
    own_h.wait()
    sib_x.wait()
    sib_h.wait()
    square_load(hint_proj).wait()

    @pl.when(core == 1)
    def _():
        u_ref[...] = (u_ref[...].astype(F32) + mat_f32(t_ref[...], wo_ref[...])).astype(BF16)

    square_load(blocks[0][1]).start()
    skip_load(0).start()

    def run_block(number, span, share, norm):
        w_qkv, w_proj, w_up, w_down = blocks[number]
        lanes = pl.ds(0, span)
        per_q = q_tile // span
        q_tiles = chips // per_q
        per_chunk = chunk // span
        rows_all = slice(0, span)

        def q_copy(off):
            return to_device(x_buf.at[ahead(off), 0, :, lanes], q_in.at[off, :, lanes], q_send.at[off], q_recv.at[off], 2 * ahead(off) + core)

        def kv_copy(off):
            return to_device(x_buf.at[ahead(off), pl.ds(1, 2), :, lanes], kv_in.at[off, :, :, lanes], kv_send.at[off], kv_recv.at[off], 2 * ahead(off) + core)

        def o_copy(off):
            return to_device(o_buf.at[off, :, lanes], back_ref.at[chip, :, lanes], o_send.at[off], o_recv.at[off], 2 * behind(off) + core)

        def sib_copy(off):
            return to_device(kv_in.at[off, :, :, lanes], kv_in.at[off, :, :, pl.ds(span, span)], sib_send.at[off], sib_recv.at[off], sibling)

        own_q = pltpu.make_async_copy(x_buf.at[chip, 0, :, lanes], q_in.at[0, :, lanes], own_sem.at[0])
        own_kv = pltpu.make_async_copy(x_buf.at[chip, pl.ds(1, 2), :, lanes], kv_in.at[0, :, :, lanes], own_sem.at[1])
        own_o = pltpu.make_async_copy(o_buf.at[0, :, lanes], back_ref.at[chip, :, lanes], own_sem.at[2])

        t_ref[rows_all, :] = layer_norm(u_ref[rows_all, :], norm[0:1], norm[1:2])

        def product(part):
            qkv_load(w_qkv, part).wait()
            prod = mat_f32(t_ref[rows_all, :], wqkv_ref[:, part * width:(part + 1) * width]).T
            x_buf[:, part, :, rows_all] = prod.reshape(heads, head_dim, span).astype(BF16)

        product(1)
        product(2)
        own_kv.start()
        if not share:
            for off in range(1, chips):
                kv_copy(off).start()
        product(0)
        own_q.start()
        for off in range(1, per_q):
            q_copy(off).start()
        if share:
            for off in range(1, chips):
                kv_copy(off).start()
        for off in range(per_q, chips):
            q_copy(off).start()
        if number + 1 < len(blocks):
            start_qkv(blocks[number + 1][0])

        ones_row = (lax.broadcasted_iota(jnp.int32, (v_rows - head_dim, span), 0) == 0).astype(F32)
        low_peak = jnp.full((8, q_tile), -jnp.inf, F32)

        def fill_q(dst, src, part):
            wide = q_in[src, :, rows_all].astype(F32) * scale
            high = wide.astype(BF16).astype(F32)
            dst[:, part * span:(part + 1) * span] = jnp.concatenate([high, wide - high], axis=0).astype(BF16)

        def score(dst, rows, q2, peak):
            part = mat_f32(k2_ref[rows, :], q2)
            dst[rows, :] = part
            return jnp.maximum(peak, jnp.max(part.reshape(part.shape[0] // 8, 8, q_tile), axis=0))

        def take_kv(src, first_lane, place, peak):
            key_t = kv_in[src, 0, :, first_lane:first_lane + span].astype(F32)
            rows = pl.ds(pl.multiple_of(place * span, span), span)
            k2_ref[rows, :] = jnp.concatenate([key_t, key_t], axis=0).T.astype(BF16)
            val_t = jnp.concatenate([kv_in[src, 1, :, first_lane:first_lane + span].astype(F32), ones_row], axis=0).astype(BF16)
            v_ref[place // per_chunk, :, pl.ds(pl.multiple_of(lax.rem(place, per_chunk) * span, span), span)] = val_t
            return score(sa_ref, rows, q2a_ref[...], peak)

        own_q.wait()
        own_kv.wait()
        fill_q(q2a_ref, 0, 0)
        if share:
            if number > layers + 1:
                pl.semaphore_wait(credit_sem, 1)
            sib_copy(0).start()
        for off in range(1, per_q):
            q_copy(off).wait_recv()
            fill_q(q2a_ref, off, off)
        peak = take_kv(0, 0, 0, low_peak)

        def arrive(off, peak):
            kv_copy(off).wait_recv()
            if share:
                sib_copy(off).start()
            return take_kv(off, 0, off, peak)

        peak = lax.fori_loop(1, chips, arrive, peak)
        if share:
            def arrive_sib(off, peak):
                sib_copy(off).wait_recv()
                return take_kv(off, span, chips + off, peak)

            peak = lax.fori_loop(0, chips, arrive_sib, peak)

            def sent_sib(off, carry):
                sib_copy(off).wait_send()
                return carry

            lax.fori_loop(0, chips, sent_sib, 0)
            if number + 1 < len(blocks):
                pl.semaphore_signal(credit_sem, inc=1, device_id={"group": sibling}, device_id_type=MESH)

        def one_tile(tile, q2_ref, cur_ref, nxt_ref, peak):
            @pl.when(tile > 1)
            def _():
                for sub in range(per_q):
                    o_copy((tile - 1) * per_q + sub).start()

            @pl.when(tile < q_tiles - 1)
            def _():
                for sub in range(per_q):
                    off = (tile + 1) * per_q + sub
                    q_copy(off).wait_recv()
                    fill_q(q2_ref, off, sub)

            top = jnp.max(peak, axis=0, keepdims=True)
            acc = jnp.zeros((v_rows, q_tile), F32)
            new_peak = low_peak
            q2 = q2_ref[...]
            for idx in range(chunks):
                rows = slice(idx * chunk, (idx + 1) * chunk)
                new_peak = score(nxt_ref, rows, q2, new_peak)
                probs = jnp.exp2(cur_ref[rows, :] - top).astype(BF16)
                acc = acc + mat_f32(v_ref[idx], probs)
            normed = (acc[:head_dim] / acc[head_dim:head_dim + 1]).astype(BF16)
            for sub in range(per_q):
                o_buf[tile * per_q + sub, :, rows_all] = normed[:, sub * span:(sub + 1) * span]
            return new_peak

        def two_tiles(pair, peak):
            peak = one_tile(2 * pair, q2b_ref, sa_ref, sb_ref, peak)
            return one_tile(2 * pair + 1, q2a_ref, sb_ref, sa_ref, peak)

        lax.fori_loop(0, q_tiles // 2, two_tiles, peak)
        own_o.start()
        for off in range(1, per_q):
            o_copy(off).start()
        for off in range(chips - per_q, chips):
            o_copy(off).start()
        own_o.wait()

        def finish(off, carry):
            q_copy(off).wait_send()
            kv_copy(off).wait_send()
            o_copy(off).wait_send()
            o_copy(off).wait_recv()
            return carry

        lax.fori_loop(1, chips, finish, 0)

        att = back_ref[:, :, rows_all].astype(F32).reshape(width, span).T.astype(BF16)
        square_load(w_proj).wait()
        res = (u_ref[rows_all, :].astype(F32) + mat_f32(att, wo_ref[...])).astype(BF16)
        u_ref[rows_all, :] = res
        if number <= layers:
            square_load(zero_proj.at[number]).start()
        elif number + 1 < len(blocks):
            square_load(blocks[number + 1][1]).start()
        else:
            square_load(w_out).start()
        t_ref[rows_all, :] = layer_norm(res, norm[2:3], norm[3:4])
        acc_ref[rows_all, :] = jnp.zeros((span, width), F32)

        def mlp(part, carry):
            cols = pl.ds(pl.multiple_of(part * tile_w, tile_w), tile_w)
            up_load(w_up, part).wait()
            hidden = jax.nn.gelu(mat_f32(t_ref[rows_all, :], w1_ref[:, cols]), approximate=True).astype(BF16)
            down_load(w_down, part).wait()
            acc_ref[rows_all, :] += mat_f32(hidden, w2_ref[cols, :])
            return carry

        lax.fori_loop(0, mlp_tiles, mlp, 0)
        u_ref[rows_all, :] = (u_ref[rows_all, :].astype(F32) + acc_ref[rows_all, :]).astype(BF16)
        if number + 1 < len(blocks):
            start_mlp(blocks[number + 1][2], blocks[number + 1][3])

    def pair_copy(i):
        return to_device(give_ref.at[i], got_ref.at[i], pair_send.at[2 + i], pair_recv.at[2 + i], sibling)

    for i in range(layers + 1):
        run_block(i, 2 * slab, False, in_norm[core, i].astype(F32))
        square_load(zero_proj.at[i]).wait()

        @pl.when(core == 0)
        def _():
            keep_ref[i] = u_ref[:slab, :]
            give_ref[i] = u_ref[slab:, :]

        @pl.when(core == 1)
        def _():
            ctrl = mat_f32(u_ref[...], wo_ref[...]).astype(BF16)
            keep_ref[i] = ctrl[slab:]
            give_ref[i] = ctrl[:slab]

        square_load(blocks[i + 1][1]).start()
        pair_copy(i).start()

    def both(i):
        pair_copy(i).wait()
        return (keep_ref[i].astype(F32) + got_ref[i].astype(F32)).astype(BF16)

    for i in range(layers):
        state = both(layers) if i == 0 else u_ref[:slab, :]
        skip_val = both(layers - 1 - i)
        skip_load(i).wait()
        merged = mat_f32(state, ws_ref[:width, :]) + mat_f32(skip_val, ws_ref[width:, :])
        u_ref[:slab, :] = merged.astype(BF16)
        if i + 1 < layers:
            skip_load(i + 1).start()
        run_block(layers + 1 + i, slab, True, out_norm[i].astype(F32))

    last = final_norm[...].astype(F32)
    square_load(w_out).wait()
    y_ref[...] = mat_f32(layer_norm(u_ref[:slab, :], last[0:1], last[1:2]), wo_ref[...]).astype(BF16)


def solution(mesh):
    chips = mesh.shape["group"] // 2
    chunk, q_tile = 512, 256

    def device_step(x_own, hint_own, in_qkv, in_proj, in_up, in_down, in_norm, out_qkv, out_proj, out_up, out_down, out_norm, zero_proj, hint_proj, skip_proj, final_norm, w_out):
        layers = skip_proj.shape[0]
        slab, width = x_own.shape
        hidden = in_up.shape[-1]
        heads = in_proj.shape[2]
        assert heads == chips
        head_dim = width // heads
        tokens = 2 * slab
        keys = chips * tokens
        v_rows = head_dim + 8
        in_proj = in_proj.reshape(in_proj.shape[:2] + (width, width))
        out_proj = out_proj.reshape((layers, width, width))
        mlp_tiles = hidden // width
        vmem, dma = pltpu.VMEM, pltpu.SemaphoreType.DMA
        in_vmem, anywhere = pl.BlockSpec(memory_space=pltpu.VMEM), pl.BlockSpec(memory_space=pl.ANY)
        specs = [anywhere] * 17
        for place in (6, 11, 15):
            specs[place] = in_vmem
        return pl.pallas_call(
            functools.partial(step_kernel, heads=heads, chunk=chunk, q_tile=q_tile),
            in_specs=specs,
            out_specs=in_vmem,
            out_shape=jax.ShapeDtypeStruct((slab, width), BF16),
            scratch_shapes=[
                vmem((width, 3 * width), BF16), vmem((width, width), BF16), vmem((width, hidden), BF16), vmem((hidden, width), BF16),
                vmem((2 * width, width), BF16),
                vmem((tokens, width), BF16), vmem((tokens, width), BF16), vmem((tokens, width), F32),
                vmem((chips, 3, head_dim, tokens), BF16), vmem((chips, head_dim, tokens), BF16), vmem((chips, 2, head_dim, tokens), BF16),
                vmem((chips, head_dim, tokens), BF16), vmem((chips, head_dim, tokens), BF16),
                vmem((2 * head_dim, q_tile), BF16), vmem((2 * head_dim, q_tile), BF16),
                vmem((keys, 2 * head_dim), BF16), vmem((keys // chunk, v_rows, chunk), BF16),
                vmem((keys, q_tile), F32), vmem((keys, q_tile), F32),
                vmem((layers + 1, slab, width), BF16), vmem((layers + 1, slab, width), BF16), vmem((layers + 1, slab, width), BF16),
                dma((3,)), dma, dma((mlp_tiles,)), dma((mlp_tiles,)), dma,
            ] + [dma((chips,))] * 8 + [dma((layers + 3,)), dma((layers + 3,)), dma((3,)), pltpu.SemaphoreType.REGULAR],
            compiler_params=pltpu.CompilerParams(collective_id=0, has_side_effects=True, vmem_limit_bytes=VMEM_LIMIT),
            name="denoiser_step",
        )(x_own, hint_own, in_qkv, in_proj, in_up, in_down, in_norm, out_qkv, out_proj, out_up, out_down, out_norm,
          zero_proj, hint_proj, skip_proj, final_norm, w_out)

    tok_spec = P(("data", "group"), None)
    return jax.shard_map(device_step, mesh=mesh, in_specs=(tok_spec, tok_spec) + (P(),) * 15, out_specs=tok_spec, check_vma=False)
```

```python
import functools
import math
import jax
import jax.numpy as jnp
from jax import lax
from jax.experimental import pallas as pl
from jax.experimental.pallas import tpu as pltpu
from jax.sharding import PartitionSpec as P

EPS = 1e-6
LOG2E = 1.4426950408889634
F32 = jnp.float32
BF16 = jnp.bfloat16
VMEM_LIMIT = 67043328
MESH = pl.DeviceIdType.MESH


def mat_f32(left_op, right_op):
    return jnp.dot(left_op, right_op, preferred_element_type=F32)


def layer_norm(values, norm_gain, norm_shift):
    wide_vals = values.astype(F32)
    centered = wide_vals - jnp.mean(wide_vals, axis=-1, keepdims=True)
    variance = jnp.mean(centered * centered, axis=-1, keepdims=True)
    normed = centered * lax.rsqrt(variance + EPS)
    return (normed * norm_gain + norm_shift).astype(BF16)


def step_kernel(x_hbm, hint_hbm, in_qkv, in_proj, in_up, in_down, in_norm, out_qkv, out_proj, out_up, out_down, out_norm,
                zero_proj, hint_proj, skip_proj, final_norm, w_out, y_ref,
                wqkv_ref, wo_ref, w1_ref, w2_ref, ws_ref, u_ref, t_ref, acc_ref, x_buf, q_in, kv_in, o_buf, back_ref,
                q2a_ref, q2b_ref, k2_ref, v_ref, sa_ref, sb_ref, keep_ref, give_ref, got_ref,
                wqkv_sem, wo_sem, w1_sem, w2_sem, ws_sem, q_send, q_recv, kv_send, kv_recv, o_send, o_recv, sib_send, sib_recv,
                pair_send, pair_recv, own_sem, credit_sem, *, heads, chunk, q_tile):
    chips = heads
    side = math.isqrt(chips)
    width = u_ref.shape[1]
    head_dim = width // heads
    slab = x_hbm.shape[0]
    layers = skip_proj.shape[0]
    me = lax.axis_index("group")
    chip, core = me // 2, lax.rem(me, 2)
    sibling = me + 1 - 2 * core
    v_rows = v_ref.shape[1]
    chunks = k2_ref.shape[0] // chunk
    scale = head_dim ** -0.5 * LOG2E
    tile_w = width
    mlp_tiles = w1_ref.shape[1] // tile_w

    row, col = chip // side, lax.rem(chip, side)

    def ahead(off):
        return lax.rem(row + off // side, side) * side + lax.rem(col + off % side, side)

    def behind(off):
        return lax.rem(row + side - off // side, side) * side + lax.rem(col + side - off % side, side)

    def to_device(src, dst, send, recv, device):
        return pltpu.make_async_remote_copy(
            src_ref=src, dst_ref=dst, send_sem=send, recv_sem=recv, device_id={"group": device}, device_id_type=MESH)

    def qkv_load(src, part):
        cols = pl.ds(part * width, width)
        return pltpu.make_async_copy(src.at[:, cols], wqkv_ref.at[:, cols], wqkv_sem.at[part])

    def square_load(src):
        return pltpu.make_async_copy(src, wo_ref, wo_sem)

    def up_load(src, part):
        cols = pl.ds(part * tile_w, tile_w)
        return pltpu.make_async_copy(src.at[:, cols], w1_ref.at[:, cols], w1_sem.at[part])

    def down_load(src, part):
        rows = pl.ds(part * tile_w, tile_w)
        return pltpu.make_async_copy(src.at[rows], w2_ref.at[rows], w2_sem.at[part])

    def skip_load(layer):
        return pltpu.make_async_copy(skip_proj.at[layer], ws_ref, ws_sem)

    def start_qkv(src):
        for part in (1, 2, 0):
            qkv_load(src, part).start()

    def start_mlp(up, down):
        for part in range(mlp_tiles):
            up_load(up, part).start()
            down_load(down, part).start()

    def in_block(i):
        return in_qkv.at[core, i], in_proj.at[core, i], in_up.at[core, i], in_down.at[core, i]

    def out_block(i):
        return out_qkv.at[i], out_proj.at[i], out_up.at[i], out_down.at[i]

    sem = pltpu.get_barrier_semaphore()
    greeted = [2 * ahead(off) + core for off in range(1, chips)] + [sibling]
    for peer in greeted:
        pl.semaphore_signal(sem, inc=1, device_id={"group": peer}, device_id_type=MESH)
    mine = pl.ds(pl.multiple_of(core * slab, slab), slab)
    own_x = pltpu.make_async_copy(x_hbm, u_ref.at[mine], own_sem.at[0])
    own_h = pltpu.make_async_copy(hint_hbm, t_ref.at[mine], own_sem.at[1])
    own_x.start()
    own_h.start()
    square_load(hint_proj).start()
    start_qkv(in_block(0)[0])
    start_mlp(*in_block(0)[2:])
    pl.semaphore_wait(sem, len(greeted))
    sib_x = to_device(x_hbm, u_ref.at[mine], pair_send.at[0], pair_recv.at[0], sibling)
    sib_h = to_device(hint_hbm, t_ref.at[mine], pair_send.at[1], pair_recv.at[1], sibling)
    sib_x.start()
    sib_h.start()
    own_x.wait()
    own_h.wait()
    sib_x.wait()
    sib_h.wait()
    square_load(hint_proj).wait()

    @pl.when(core == 1)
    def _():
        u_ref[...] = (u_ref[...].astype(F32) + mat_f32(t_ref[...], wo_ref[...])).astype(BF16)

    square_load(in_block(0)[1]).start()
    skip_load(0).start()

    def run_block(i, weights, span, share, norm, next_qkv, next_square, next_mlp):
        w_qkv, w_proj, w_up, w_down = weights
        lanes = pl.ds(0, span)
        per_q = q_tile // span
        q_tiles = chips // per_q
        per_chunk = chunk // span
        rows_all = slice(0, span)

        def q_copy(off):
            return to_device(x_buf.at[ahead(off), 0, :, lanes], q_in.at[off, :, lanes], q_send.at[off], q_recv.at[off], 2 * ahead(off) + core)

        def kv_copy(off):
            return to_device(x_buf.at[ahead(off), pl.ds(1, 2), :, lanes], kv_in.at[off, :, :, lanes], kv_send.at[off], kv_recv.at[off], 2 * ahead(off) + core)

        def send_kv():
            for off in range(1, chips):
                kv_copy(off).start()

        def o_copy(off):
            return to_device(o_buf.at[off, :, lanes], back_ref.at[chip, :, lanes], o_send.at[off], o_recv.at[off], 2 * behind(off) + core)

        def sib_copy(off):
            return to_device(kv_in.at[off, :, :, lanes], kv_in.at[off, :, :, pl.ds(span, span)], sib_send.at[off], sib_recv.at[off], sibling)

        own_q = pltpu.make_async_copy(x_buf.at[chip, 0, :, lanes], q_in.at[0, :, lanes], own_sem.at[0])
        own_kv = pltpu.make_async_copy(x_buf.at[chip, pl.ds(1, 2), :, lanes], kv_in.at[0, :, :, lanes], own_sem.at[1])
        own_o = pltpu.make_async_copy(o_buf.at[0, :, lanes], back_ref.at[chip, :, lanes], own_sem.at[2])

        t_ref[rows_all, :] = layer_norm(u_ref[rows_all, :], norm[0:1], norm[1:2])

        def product(part):
            qkv_load(w_qkv, part).wait()
            prod = mat_f32(t_ref[rows_all, :], wqkv_ref[:, part * width:(part + 1) * width]).T
            x_buf[:, part, :, rows_all] = prod.reshape(heads, head_dim, span).astype(BF16)

        product(1)
        product(2)
        own_kv.start()
        if not share:
            send_kv()
        product(0)
        own_q.start()
        for off in range(1, per_q):
            q_copy(off).start()
        if share:
            send_kv()
        for off in range(per_q, chips):
            q_copy(off).start()
        next_qkv()

        ones_row = (lax.broadcasted_iota(jnp.int32, (v_rows - head_dim, span), 0) == 0).astype(F32)
        low_peak = jnp.full((8, q_tile), -jnp.inf, F32)

        def fill_q(dst, src, part):
            wide = q_in[src, :, rows_all].astype(F32) * scale
            high = wide.astype(BF16).astype(F32)
            dst[:, part * span:(part + 1) * span] = jnp.concatenate([high, wide - high], axis=0).astype(BF16)

        def score(dst, rows, q2, peak):
            part = mat_f32(k2_ref[rows, :], q2)
            dst[rows, :] = part
            return jnp.maximum(peak, jnp.max(part.reshape(part.shape[0] // 8, 8, q_tile), axis=0))

        batch = 2 * per_q

        def take_batch(first, first_lane, place, peak):
            for sub in range(batch):
                key_t = kv_in[first + sub, 0, :, first_lane:first_lane + span].astype(F32)
                rows = pl.ds(pl.multiple_of((place + sub) * span, span), span)
                k2_ref[rows, :] = jnp.concatenate([key_t, key_t], axis=0).T.astype(BF16)
                val_t = jnp.concatenate([kv_in[first + sub, 1, :, first_lane:first_lane + span].astype(F32), ones_row], axis=0).astype(BF16)
                lane = pl.multiple_of(lax.rem(place + sub, per_chunk) * span, span)
                v_ref[(place + sub) // per_chunk, :, pl.ds(lane, span)] = val_t
            batch_rows = pl.ds(pl.multiple_of(place * span, batch * span), batch * span)
            return score(sa_ref, batch_rows, q2a_ref[...], peak)

        own_q.wait()
        own_kv.wait()
        fill_q(q2a_ref, 0, 0)
        if share:
            @pl.when(i > 0)
            def _():
                pl.semaphore_wait(credit_sem, 1)

            sib_copy(0).start()
        for off in range(1, per_q):
            q_copy(off).wait_recv()
            fill_q(q2a_ref, off, off)
        def arrive(step, peak):
            first = step * batch

            @pl.when(step > 0)
            def _():
                kv_copy(first).wait_recv()
                if share:
                    sib_copy(first).start()

            for sub in range(1, batch):
                kv_copy(first + sub).wait_recv()
                if share:
                    sib_copy(first + sub).start()
            return take_batch(first, 0, first, peak)

        peak = lax.fori_loop(0, chips // batch, arrive, low_peak)
        if share:
            def arrive_sib(step, peak):
                first = step * batch
                for sub in range(batch):
                    sib_copy(first + sub).wait_recv()
                return take_batch(first, span, chips + first, peak)

            peak = lax.fori_loop(0, chips // batch, arrive_sib, peak)

            def sent_sib(off, carry):
                sib_copy(off).wait_send()
                return carry

            lax.fori_loop(0, chips, sent_sib, 0)

            @pl.when(i < layers - 1)
            def _():
                pl.semaphore_signal(credit_sem, inc=1, device_id={"group": sibling}, device_id_type=MESH)

        def one_tile(tile, q2_ref, cur_ref, nxt_ref, peak):
            @pl.when(tile > 1)
            def _():
                for sub in range(per_q):
                    o_copy((tile - 1) * per_q + sub).start()

            @pl.when(tile < q_tiles - 1)
            def _():
                for sub in range(per_q):
                    off = (tile + 1) * per_q + sub
                    q_copy(off).wait_recv()
                    fill_q(q2_ref, off, sub)

            top = jnp.max(peak, axis=0, keepdims=True)
            acc = jnp.zeros((v_rows, q_tile), F32)
            new_peak = low_peak
            q2 = q2_ref[...]
            for idx in range(chunks):
                rows = slice(idx * chunk, (idx + 1) * chunk)
                new_peak = score(nxt_ref, rows, q2, new_peak)
                probs = jnp.exp2(cur_ref[rows, :] - top).astype(BF16)
                acc = acc + mat_f32(v_ref[idx], probs)
            normed = (acc[:head_dim] / acc[head_dim:head_dim + 1]).astype(BF16)
            for sub in range(per_q):
                o_buf[tile * per_q + sub, :, rows_all] = normed[:, sub * span:(sub + 1) * span]
            return new_peak

        def two_tiles(pair, peak):
            peak = one_tile(2 * pair, q2b_ref, sa_ref, sb_ref, peak)
            return one_tile(2 * pair + 1, q2a_ref, sb_ref, sa_ref, peak)

        lax.fori_loop(0, q_tiles // 2, two_tiles, peak)
        own_o.start()
        for off in range(1, per_q):
            o_copy(off).start()
        for off in range(chips - per_q, chips):
            o_copy(off).start()
        own_o.wait()

        def finish(off, carry):
            q_copy(off).wait_send()
            kv_copy(off).wait_send()
            o_copy(off).wait_send()
            o_copy(off).wait_recv()
            return carry

        lax.fori_loop(1, chips, finish, 0)

        att = back_ref[:, :, rows_all].astype(F32).reshape(width, span).T.astype(BF16)
        square_load(w_proj).wait()
        res = (u_ref[rows_all, :].astype(F32) + mat_f32(att, wo_ref[...])).astype(BF16)
        u_ref[rows_all, :] = res
        next_square()
        t_ref[rows_all, :] = layer_norm(res, norm[2:3], norm[3:4])
        for part in range(mlp_tiles):
            up_load(w_up, part).wait()
            down_load(w_down, part).wait()
        for part in range(mlp_tiles):
            cols = slice(part * tile_w, (part + 1) * tile_w)
            hidden = jax.nn.gelu(mat_f32(t_ref[rows_all, :], w1_ref[:, cols]), approximate=True).astype(BF16)
            down = mat_f32(hidden, w2_ref[cols, :])
            acc_ref[rows_all, :] = down if part == 0 else acc_ref[rows_all, :] + down
        u_ref[rows_all, :] = (u_ref[rows_all, :].astype(F32) + acc_ref[rows_all, :]).astype(BF16)
        next_mlp()

    def pair_copy(i):
        return to_device(give_ref.at[i], got_ref.at[i], pair_send.at[2 + i], pair_recv.at[2 + i], sibling)

    def either(test, yes, no):
        pl.when(test)(yes)
        pl.when(jnp.logical_not(test))(no)

    def in_step(i, carry):
        run_block(
            i, in_block(i), 2 * slab, False, in_norm[core, i].astype(F32),
            lambda: either(i < layers, lambda: start_qkv(in_block(i + 1)[0]), lambda: start_qkv(out_block(0)[0])),
            lambda: square_load(zero_proj.at[i]).start(),
            lambda: either(i < layers, lambda: start_mlp(*in_block(i + 1)[2:]), lambda: start_mlp(*out_block(0)[2:])),
        )
        square_load(zero_proj.at[i]).wait()

        @pl.when(core == 0)
        def _():
            keep_ref[i] = u_ref[:slab, :]
            give_ref[i] = u_ref[slab:, :]

        @pl.when(core == 1)
        def _():
            ctrl = mat_f32(u_ref[...], wo_ref[...]).astype(BF16)
            keep_ref[i] = ctrl[slab:]
            give_ref[i] = ctrl[:slab]

        either(i < layers, lambda: square_load(in_block(i + 1)[1]).start(), lambda: square_load(out_block(0)[1]).start())
        pair_copy(i).start()
        return carry

    lax.fori_loop(0, layers + 1, in_step, 0)

    def both(i):
        pair_copy(i).wait()
        return (keep_ref[i].astype(F32) + got_ref[i].astype(F32)).astype(BF16)

    u_ref[:slab, :] = both(layers)

    def out_step(i, carry):
        skip_val = both(layers - 1 - i)
        skip_load(i).wait()
        merged = mat_f32(u_ref[:slab, :], ws_ref[:width, :]) + mat_f32(skip_val, ws_ref[width:, :])
        u_ref[:slab, :] = merged.astype(BF16)
        more = i < layers - 1
        pl.when(more)(lambda: skip_load(i + 1).start())
        run_block(
            i, out_block(i), slab, True, out_norm[i].astype(F32),
            lambda: pl.when(more)(lambda: start_qkv(out_block(i + 1)[0])),
            lambda: either(more, lambda: square_load(out_block(i + 1)[1]).start(), lambda: square_load(w_out).start()),
            lambda: pl.when(more)(lambda: start_mlp(*out_block(i + 1)[2:])),
        )
        return carry

    lax.fori_loop(0, layers, out_step, 0)

    last = final_norm[...].astype(F32)
    square_load(w_out).wait()
    y_ref[...] = mat_f32(layer_norm(u_ref[:slab, :], last[0:1], last[1:2]), wo_ref[...]).astype(BF16)


def solution(mesh):
    chips = mesh.shape["group"] // 2
    chunk, q_tile = 512, 256

    def device_step(x_own, hint_own, in_qkv, in_proj, in_up, in_down, in_norm, out_qkv, out_proj, out_up, out_down, out_norm, zero_proj, hint_proj, skip_proj, final_norm, w_out):
        layers = skip_proj.shape[0]
        slab, width = x_own.shape
        hidden = in_up.shape[-1]
        heads = in_proj.shape[2]
        assert heads == chips
        head_dim = width // heads
        tokens = 2 * slab
        keys = chips * tokens
        v_rows = head_dim + 8
        in_proj = in_proj.reshape(in_proj.shape[:2] + (width, width))
        out_proj = out_proj.reshape((layers, width, width))
        mlp_tiles = hidden // width
        vmem, dma = pltpu.VMEM, pltpu.SemaphoreType.DMA
        in_vmem, anywhere = pl.BlockSpec(memory_space=pltpu.VMEM), pl.BlockSpec(memory_space=pl.ANY)
        specs = [anywhere] * 17
        for place in (6, 11, 15):
            specs[place] = in_vmem
        return pl.pallas_call(
            functools.partial(step_kernel, heads=heads, chunk=chunk, q_tile=q_tile),
            in_specs=specs,
            out_specs=in_vmem,
            out_shape=jax.ShapeDtypeStruct((slab, width), BF16),
            scratch_shapes=[
                vmem((width, 3 * width), BF16), vmem((width, width), BF16), vmem((width, hidden), BF16), vmem((hidden, width), BF16),
                vmem((2 * width, width), BF16),
                vmem((tokens, width), BF16), vmem((tokens, width), BF16), vmem((tokens, width), F32),
                vmem((chips, 3, head_dim, tokens), BF16), vmem((chips, head_dim, tokens), BF16), vmem((chips, 2, head_dim, tokens), BF16),
                vmem((chips, head_dim, tokens), BF16), vmem((chips, head_dim, tokens), BF16),
                vmem((2 * head_dim, q_tile), BF16), vmem((2 * head_dim, q_tile), BF16),
                vmem((keys, 2 * head_dim), BF16), vmem((keys // chunk, v_rows, chunk), BF16),
                vmem((keys, q_tile), F32), vmem((keys, q_tile), F32),
                vmem((layers + 1, slab, width), BF16), vmem((layers + 1, slab, width), BF16), vmem((layers + 1, slab, width), BF16),
                dma((3,)), dma, dma((mlp_tiles,)), dma((mlp_tiles,)), dma,
            ] + [dma((chips,))] * 8 + [dma((layers + 3,)), dma((layers + 3,)), dma((3,)), pltpu.SemaphoreType.REGULAR],
            compiler_params=pltpu.CompilerParams(collective_id=0, has_side_effects=True, vmem_limit_bytes=VMEM_LIMIT),
            name="denoiser_step",
        )(x_own, hint_own, in_qkv, in_proj, in_up, in_down, in_norm, out_qkv, out_proj, out_up, out_down, out_norm,
          zero_proj, hint_proj, skip_proj, final_norm, w_out)

    tok_spec = P(("data", "group"), None)
    return jax.shard_map(device_step, mesh=mesh, in_specs=(tok_spec, tok_spec) + (P(),) * 15, out_specs=tok_spec, check_vma=False)
```
